32 devices in a mesh: pb: 4 (over z), freq: 4 (over y, core), ga: 2 (over x).
Axes of the slice: x: 2, y: 2, z: 4, core: 2. Of those that a mesh axis runs over, the one named last changes fastest.
Arguments:
- densities: bfloat16 [4, 2, 256, 4096], P('pb', None, ('freq', 'ga')), may hold values from -0.5 to 0.5
- screened: bfloat16 [4, 4, 2, 4096, 4096], P('pb', 'freq', None, 'ga'), may hold values from -0.09375 to 0.09375
- energies: float32 [16, 256], replicated, may hold values from -2.5 to 2.5
- occupied: int32 [16], replicated, may hold values from 64 to 192
- kmq: int32 [4], replicated, may hold values from 0 to 15
- offsets: int32 [4], replicated, may hold values from -16 to 15
- weights: float32 [4], replicated, may hold values from 0.5 to 2
Outputs:
- sigma: float32 [2, 1, 64], P(None, None, ('pb', 'freq'))
The draws below stay inside these ranges and needn't reach their ends.
All inputs are finite; a program needn't handle non-finite values.
Results may differ from the reference program's by a relative error of at most 0.0003.
Values may be sent and summed in bfloat16 or wider, within the bound.
A program may use at most 64 MiB of HBM per device.

```python
import math
import jax
import jax.numpy as jnp
from jax import lax

G = 4096
NB = 256
NS = 1
Q = 4
NKP = 16
NW = 4
NOUT = 64
K = 256


def place_ends(result, stream_key, least, high):
    longest = result.shape.index(max(result.shape))
    spots = []
    for shift in (0, 1):
        where = [jax.random.randint(jax.random.fold_in(stream_key, axis), (), 0, length) for axis, length in enumerate(result.shape)]
        where[longest] = (where[longest] + shift) % result.shape[longest]
        spots.append(tuple(where))
    return result.at[spots[0]].set(least).at[spots[1]].set(high)


def block_scale(rng, shape, split, least, top_value):
    def one(dim, blocks):
        steps = jax.random.uniform(jax.random.fold_in(jax.random.fold_in(rng, 6), dim), (blocks,), jnp.float32, least / len(split), top_value / len(split))
        return jnp.repeat(jnp.exp(steps), shape[dim] // blocks).reshape((-1,) + (1,) * (len(shape) - dim - 1))

    factor_of = one(*split[0])
    for cut in split[1:]:
        factor_of = factor_of * one(*cut)
    return factor_of


def centred(key, shape, width, reach, pieces=(), kind=jnp.bfloat16):
    result = width * jax.random.normal(key, shape, jnp.float32)
    if pieces:
        result = result * block_scale(key, shape, pieces, -0.22, 0.18)
    return jnp.clip(result, -reach, reach).astype(kind)


def setup_inputs(seed: int = 0) -> dict:
    key_list = jax.random.split(jax.random.key(seed), 8)
    return {
        "densities": centred(key_list[0], (Q, 2, K, G), (0.7071 * G ** -0.25), 0.5, ((0, 4), (2, 8))),
        "screened": centred(key_list[1], (Q, NW, 2, G, G), G ** -0.5, 0.09375, ((0, 4), (1, 4), (3, 2))),
        "energies": jnp.clip(jax.random.uniform(key_list[2], (NKP, NB), jnp.float32, -2.5, 2.5), -2.5, 2.5),
        "occupied": place_ends(jax.random.randint(key_list[3], (NKP,), NB // 4, 3 * NB // 4 + 1), jax.random.fold_in(key_list[3], 1), NB // 4, (3 * NB // 4 + 1) - 1).astype(jnp.int32),
        "kmq": place_ends(jax.random.randint(key_list[4], (Q,), 0, NKP), jax.random.fold_in(key_list[4], 1), 0, NKP - 1).astype(jnp.int32),
        "offsets": place_ends(jax.random.randint(key_list[5], (NW,), 0 - NOUT // 4, NOUT // 4), jax.random.fold_in(key_list[5], 1), 0 - NOUT // 4, (NOUT // 4) - 1).astype(jnp.int32),
        "weights": jnp.clip(jnp.exp(jax.random.uniform(key_list[6], (NW,), jnp.float32, math.log(0.5), math.log(2.0))), 0.5, 2.0),
    }


broadening = 0.15


def green_parts(level_row, filled, freq_shift, omegas):
    bands = jnp.arange(level_row.shape[0], dtype=jnp.int32)
    pole_sign = jnp.where(bands < filled, -1.0, 1.0).astype(jnp.float32)
    real_part = omegas[None, :] - freq_shift - level_row[:, None]
    imag_part = broadening * pole_sign[:, None]
    denominator = real_part * real_part + imag_part * imag_part
    return real_part / denominator, -imag_part / denominator


def spectrum(pair_real, pair_imag, green_real, green_imag):
    exact = lax.Precision.HIGHEST
    real_out = jnp.dot(pair_real, green_real, precision=exact) - jnp.dot(pair_imag, green_imag, precision=exact)
    imag_out = jnp.dot(pair_real, green_imag, precision=exact) + jnp.dot(pair_imag, green_real, precision=exact)
    return real_out, imag_out


def pair_sums(density, screen):
    pair_rows = density.shape[1]
    basis_rows = screen.shape[1]
    product = lax.dot_general(density.reshape(2 * pair_rows, -1), screen.reshape(2 * basis_rows, -1),
                              (((1,), (1,)), ((), ())), preferred_element_type=jnp.float32)
    product = product.reshape(2, pair_rows, 2, basis_rows)
    real_x = product[0, :, 0] - product[1, :, 1]
    imag_x = product[0, :, 1] + product[1, :, 0]
    dense = density.astype(jnp.float32)
    real_sum = jnp.sum(dense[0] * real_x + dense[1] * imag_x, axis=1)
    imag_sum = jnp.sum(dense[0] * imag_x - dense[1] * real_x, axis=1)
    return real_sum, imag_sum


def reference(densities, screened, energies, occupied, kmq, offsets, weights):
    omegas = -2.0 + 4.0 * jnp.arange(NOUT, dtype=jnp.float32) / NOUT
    summed_real = jnp.zeros((NS, NOUT), jnp.float32)
    summed_imag = jnp.zeros((NS, NOUT), jnp.float32)
    for qpoint in range(Q):
        kpoint = kmq[qpoint]
        level_row = energies[kpoint]
        filled = occupied[kpoint]
        for frequency in range(NW):
            real_sum, imag_sum = pair_sums(densities[qpoint], screened[qpoint, frequency])
            weight_now = weights[frequency]
            real_sum = (weight_now * real_sum).reshape(NS, NB)
            imag_sum = (weight_now * imag_sum).reshape(NS, NB)
            freq_shift = 4.0 * offsets[frequency].astype(jnp.float32) / NOUT
            green_real, green_imag = green_parts(level_row, filled, freq_shift, omegas)
            real_out, imag_out = spectrum(real_sum, imag_sum, green_real, green_imag)
            summed_real = summed_real + real_out
            summed_imag = summed_imag + imag_out
    prefactor = 1.0 / (2.0 * math.pi * Q)
    return jnp.stack([-prefactor * summed_imag, prefactor * summed_real])
```

```python
import functools
import math

import jax
import jax.numpy as jnp
from jax import lax
from jax.experimental import pallas as pl
from jax.experimental.pallas import tpu as pltpu
from jax.sharding import PartitionSpec as P

MESH = pl.DeviceIdType.MESH
CHUNKS = 4
PANELS = 8
HALF = CHUNKS // 2
SLOTS = 8

NB = 256
NS = 1
OUT_DEV = 4


broadening = 0.15


def from_behind(block, axis, distance):
    devices = range(lax.axis_size(axis))
    route = [((i - distance) % len(devices), i) for i in devices]
    return lax.ppermute(block, axis, route)


def green_parts(level_row, filled, freq_shift, omegas):
    bands = jnp.arange(level_row.shape[0], dtype=jnp.int32)
    pole_sign = jnp.where(bands < filled, -1.0, 1.0).astype(jnp.float32)
    real_part = omegas[None, :] - freq_shift - level_row[:, None]
    imag_part = broadening * pole_sign[:, None]
    denominator = real_part * real_part + imag_part * imag_part
    return (real_part / denominator, -imag_part / denominator)


def spectrum(pair_real, pair_imag, green_real, green_imag):
    exact = lax.Precision.HIGHEST
    real_out = jnp.dot(pair_real, green_real, precision=exact) - jnp.dot(
        pair_imag, green_imag, precision=exact
    )
    imag_out = jnp.dot(pair_real, green_imag, precision=exact) + jnp.dot(
        pair_imag, green_real, precision=exact
    )
    return jnp.stack([real_out, imag_out])


def panel_product(density_all, screen):
    pair_rows = density_all.shape[1]
    panel_rows = screen.shape[1]
    product = lax.dot_general(
        density_all.reshape(2 * pair_rows, -1),
        screen.reshape(2 * panel_rows, -1),
        (((1,), (1,)), ((), ())),
        preferred_element_type=jnp.float32,
    )
    product = product.reshape(2, pair_rows, 2, panel_rows)
    return (product[0, :, 0] - product[1, :, 1], product[0, :, 1] + product[1, :, 0])


def plain_body(densities, screened, energies, occupied, kmq, offsets, weights):
    qpoint = lax.axis_index("pb")
    my_freq = lax.axis_index("freq")
    my_panel = lax.axis_index("ga")
    count_pb = lax.axis_size("pb")
    count_freq = lax.axis_size("freq")
    screen = screened[0, 0]
    panel_width = screen.shape[1]
    local_block = densities[0]
    whole = lax.all_gather(local_block, ("freq", "ga"), axis=1, tiled=True)
    real_x, imag_x = panel_product(whole, screen)
    own_rows = lax.dynamic_slice_in_dim(whole, my_panel * panel_width, panel_width, 2)
    dense = own_rows.astype(jnp.float32)
    real_sum = jnp.sum(dense[0] * real_x + dense[1] * imag_x, axis=1)
    imag_sum = jnp.sum(dense[0] * imag_x - dense[1] * real_x, axis=1)
    pair_total = lax.psum(jnp.stack([real_sum, imag_sum]), "ga")
    weighted = (pair_total * weights[my_freq]).reshape(2, NS, NB)
    kpoint = kmq[qpoint]
    level_row = energies[kpoint]
    filled = occupied[kpoint]
    total_out = OUT_DEV * count_pb * count_freq
    index_grid = (jnp.arange(count_pb, dtype=jnp.int32)[:, None] * count_freq + my_freq) * OUT_DEV
    index_grid = (index_grid + jnp.arange(OUT_DEV, dtype=jnp.int32)[None, :]).reshape(-1)
    omegas = -2.0 + 4.0 * index_grid.astype(jnp.float32) / total_out
    summed = jnp.zeros((2, NS, count_pb * OUT_DEV), jnp.float32)
    passed = weighted
    for rotation in range(count_freq):
        anchor = (my_freq - rotation) % count_freq
        freq_shift = 4.0 * offsets[anchor].astype(jnp.float32) / total_out
        green_real, green_imag = green_parts(level_row, filled, freq_shift, omegas)
        summed = summed + spectrum(passed[0], passed[1], green_real, green_imag)
        if rotation + 1 < count_freq:
            passed = from_behind(passed, "freq", 1)
    local_part = lax.psum_scatter(summed, "pb", scatter_dimension=2, tiled=True)
    prefactor = 1.0 / (2.0 * math.pi * count_pb)
    return jnp.stack([-prefactor * local_part[1], prefactor * local_part[0]])


def fused_kernel(
    shape,
    dens_hbm,
    screen_hbm,
    energy_hbm,
    filled_hbm,
    kmq_hbm,
    offset_hbm,
    weight_hbm,
    out_ref,
    dens,
    minus,
    panel,
    acc,
    psum,
    green,
    parts,
    energy,
    filled,
    kmq,
    offset,
    weight,
    own_sem,
    panel_sem,
    small_sem,
    send_sem,
    recv_sem,
    part_send,
    part_recv,
    ready,
):
    count_pb, count_freq, count_ga = shape
    group = count_freq * count_ga
    rows = dens.shape[3]
    width = dens.shape[4]
    cols = panel.shape[3]
    per = width // cols
    total_out = green.shape[2]
    qpoint = lax.axis_index("pb")
    freq = lax.axis_index("freq")
    x = lax.axis_index("ga")
    y, core = freq // 2, freq % 2
    ny, nx, nc = 1 - y, 1 - x, 1 - core
    at_x = {"freq": freq, "ga": nx}
    at_y = {"freq": ny * 2 + core, "ga": x}
    at_core = {"freq": y * 2 + nc, "ga": x}

    def place(yy, cc, xx):
        return (yy * 2 + cc) * count_ga + xx

    def owner(slot):
        dy, dx, dc = slot // 4, slot // 2 % 2, slot % 2
        return place((y + dy) % 2, (core + dc) % 2, (x + dx) % 2)

    barrier = pltpu.get_barrier_semaphore()
    for target in (at_x, at_y, at_core):
        pl.semaphore_signal(barrier, inc=1, device_id=target, device_id_type=MESH)

    def both_layers(semaphore):
        @pl.when(qpoint > 0)
        def _():
            pl.semaphore_signal(
                semaphore, inc=1, device_id={"pb": qpoint - 1}, device_id_type=MESH
            )

        @pl.when(qpoint < count_pb - 1)
        def _():
            pl.semaphore_signal(
                semaphore, inc=1, device_id={"pb": qpoint + 1}, device_id_type=MESH
            )

    layers = (qpoint + count_pb - 1) // count_pb + (2 * count_pb - 2 - qpoint) // count_pb
    both_layers(barrier)

    def own_copy(r):
        start = pl.multiple_of((x * HALF + r) % CHUNKS * width, width)
        return pltpu.make_async_copy(
            dens_hbm.at[0, :, :, pl.ds(start, width)], dens.at[r, 0], own_sem.at[r]
        )

    def panel_copy(n):
        start = pl.multiple_of((x * (PANELS // 2) + n) % PANELS * cols, cols)
        return pltpu.make_async_copy(
            screen_hbm.at[0, 0, :, :, pl.ds(start, cols)], panel.at[n], panel_sem.at[n]
        )

    first_own = [HALF + r for r in range(HALF)] + list(range(HALF))
    for r in range(CHUNKS):
        own_copy(r).start()
    small = [
        pltpu.make_async_copy(source, target, small_sem.at[i])
        for i, (source, target) in enumerate(
            [
                (energy_hbm, energy),
                (filled_hbm, filled),
                (kmq_hbm, kmq),
                (offset_hbm, offset),
                (weight_hbm, weight),
            ]
        )
    ]
    for copy in small:
        copy.start()
    for n in range(PANELS):
        panel_copy(n).start(priority=1)

    def remote(lane, r, slot, there, slot_there, target):
        return pltpu.make_async_remote_copy(
            src_ref=dens.at[r, slot],
            dst_ref=dens.at[there, slot_there],
            send_sem=send_sem.at[lane, r],
            recv_sem=recv_sem.at[there, slot_there],
            device_id=target,
            device_id_type=MESH,
        )

    def to_x(r):
        return remote(0, r, 0, (r + HALF) % CHUNKS, 2, at_x)

    def to_y(r):
        return remote(1, r, 0, r, 4, at_y)

    def to_core(r):
        return remote(2, r, 0, r, 1, at_core)

    def onward_y(r):
        return remote(3, r, 2, r, 6, at_y)

    def relay_x(r):
        return pltpu.make_async_remote_copy(
            src_ref=dens.at[r, 4],
            dst_ref=dens.at[r + HALF, 6],
            send_sem=send_sem.at[3, r + HALF],
            recv_sem=recv_sem.at[r + HALF, 6],
            device_id=at_x,
            device_id_type=MESH,
        )

    def share(r, slot):
        return remote(3 + slot // 2, r, slot, r, slot + 1, at_core)

    def arrived(r, slot):
        remote(0, r, slot, r, slot, at_x).wait_recv()

    def take(r, slot):
        arrived(r, slot)
        share(r, slot).start()

    def pass_ready(step):
        if step < count_pb - 1:
            pl.semaphore_wait(ready.at[step - 1], layers)
            both_layers(ready.at[step])

    def prepare(r, slots):
        for slot in slots:
            minus[r, slot] = -dens[r, slot, 1]

    with jax.named_scope("bar"):
        pl.semaphore_wait(barrier, 3 + layers)
    for r in first_own:
        with jax.named_scope(f"own{r}"):
            own_copy(r).wait()
        if r >= HALF:
            to_x(r).start()
        else:
            to_y(r).start()
        to_core(r).start()
    for r in range(HALF):
        to_x(r).start()

    with jax.named_scope("small"):
        for copy in small:
            copy.wait()
    kpoint = kmq[qpoint]
    level_row = energy[pl.ds(kpoint, 1), :]
    levels = jnp.broadcast_to(level_row, (8, level_row.shape[1])).T[:, :1]
    bands = lax.broadcasted_iota(jnp.int32, (level_row.shape[1], total_out), 0)
    grid = lax.broadcasted_iota(jnp.int32, (level_row.shape[1], total_out), 1)
    omegas = -2.0 + 4.0 * grid.astype(jnp.float32) / total_out
    freq_shift = 4.0 * offset[freq].astype(jnp.float32) / total_out
    real_part = omegas - freq_shift - levels
    imag_part = jnp.where(bands < filled[kpoint], -broadening, broadening)
    scale = weight[freq] / (2.0 * math.pi * count_pb)
    inverse = scale / (real_part * real_part + imag_part * imag_part)
    green[0] = real_part * inverse
    green[1] = -imag_part * inverse

    def product(slots, chunks, n):
        low = chunks[0] * width
        depth = len(chunks) * width
        left = []
        for plane in range(2):
            for r in chunks:
                pieces = []
                for slot in slots:
                    if plane == 0:
                        pieces += [dens[r, slot, 0], minus[r, slot]]
                    else:
                        pieces += [dens[r, slot, 1], dens[r, slot, 0]]
                left.append(jnp.concatenate(pieces, axis=0))
        right = [panel[n, plane, low : low + depth, :] for plane in range(2)]
        return lax.dot_general(
            jnp.concatenate(left, axis=1),
            jnp.concatenate(right, axis=0),
            (((1,), (0,)), ((), ())),
            preferred_element_type=jnp.float32,
        )

    started = set()

    def reduce(value, slots, n):
        r, off = n // per, n % per * cols
        for i, slot in enumerate(slots):
            real_y = value[2 * i * rows : (2 * i + 1) * rows]
            imag_y = value[(2 * i + 1) * rows : (2 * i + 2) * rows]
            real_d = dens[r, slot, 0, :, off : off + cols].astype(jnp.float32)
            imag_d = dens[r, slot, 1, :, off : off + cols].astype(jnp.float32)
            real = real_y * real_d - imag_y * imag_d
            imag = real_y * imag_d + imag_y * real_d
            for c, total in enumerate((real, imag)):
                narrow = total[:, :128]
                for part in range(1, cols // 128):
                    narrow = narrow + total[:, part * 128 : (part + 1) * 128]
                if slot in started:
                    psum[c, slot] += narrow
                else:
                    psum[c, slot] = narrow
            started.add(slot)

    def spectra(slots):
        real_out = jnp.zeros((rows, total_out), jnp.float32)
        imag_out = jnp.zeros((rows, total_out), jnp.float32)
        for slot in slots:
            pair_real = jnp.sum(psum[0, slot], axis=1, keepdims=True)
            pair_imag = jnp.sum(psum[1, slot], axis=1, keepdims=True)
            here = pl.ds(pl.multiple_of(owner(slot) * rows, rows), rows)
            green_real, green_imag = green[0, here, :], green[1, here, :]
            real_out = real_out + pair_real * green_real - pair_imag * green_imag
            imag_out = imag_out + pair_real * green_imag + pair_imag * green_real
        return real_out, imag_out

    head = list(range(HALF))
    near, far = (2, 3, 4, 5), (6, 7)

    def own_block(n):
        with jax.named_scope(f"pan{n}"):
            panel_copy(n).wait()
        reduce(product((0, 1), head, n), (0, 1), n)

    def near_first(n):
        acc[n] = product(near, [0], n)

    def near_last(n):
        value = acc[n] + product(near, [1], n)
        if n < PANELS // 2:
            reduce(value, near, n)
        else:
            reduce(value[: 4 * rows], near[:2], n)
            acc[n, 4 * rows :, :] = value[4 * rows :]

    def far_block(n):
        value = product(far, head, n)
        reduce(value, far, n)
        if n >= PANELS // 2:
            reduce(acc[n, 4 * rows :, :], near[2:], n)

    for r in head:
        prepare(r, (0,))
    with jax.named_scope("sib"):
        for r in range(CHUNKS):
            arrived(r, 1)
    for r in head:
        prepare(r, (1,))
    for n in range(4):
        own_block(n)
    with jax.named_scope("take0"):
        take(0, 2)
        onward_y(0).start()
        take(0, 4)
        relay_x(0).start()
    own_block(4)
    with jax.named_scope("got0"):
        arrived(0, 3)
        arrived(0, 5)
    prepare(0, near)
    near_first(0)
    with jax.named_scope("take1"):
        take(1, 2)
        onward_y(1).start()
        for r in range(HALF, CHUNKS):
            to_y(r).start()
        take(1, 4)
        relay_x(1).start()
    own_block(5)
    near_first(1)
    own_block(6)
    near_first(2)
    own_block(7)
    near_first(3)
    with jax.named_scope("take2"):
        take(2, 2)
        take(0, 6)
    for n in range(4, PANELS):
        near_first(n)
    with jax.named_scope("take3"):
        arrived(1, 3)
        arrived(1, 5)
        take(3, 2)
        take(1, 6)
        arrived(0, 7)
        both_layers(ready.at[0])
    prepare(1, near)
    for n in range(4):
        near_last(n)
    with jax.named_scope("take4"):
        arrived(2, 3)
        arrived(3, 3)
        take(2, 4)
        take(2, 6)
        pass_ready(1)
    for n in range(4, PANELS):
        near_last(n)
    with jax.named_scope("take5"):
        arrived(1, 7)
        take(3, 4)
        take(3, 6)
        for step in range(2, count_pb - 1):
            pass_ready(step)
    early = spectra((0, 1, 2, 3))
    for r in head:
        prepare(r, far)
    for n in range(4):
        far_block(n)
    with jax.named_scope("last"):
        for r in range(HALF, CHUNKS):
            arrived(r, 5)
            arrived(r, 7)
    for n in range(4, PANELS):
        far_block(n)
    final = spectra((4, 5, 6, 7))
    parts[0, 0:1] = -jnp.sum(early[1] + final[1], axis=0, keepdims=True)
    parts[0, 1:2] = jnp.sum(early[0] + final[0], axis=0, keepdims=True)
    with jax.named_scope("ready"):
        pl.semaphore_wait(ready.at[count_pb - 2], layers)
    me = owner(0)
    copies = []
    for step in range(1, count_pb * group):
        spot = (me + step) % group
        target = {
            "pb": (qpoint + step // group) % count_pb,
            "freq": spot // count_ga,
            "ga": spot % count_ga,
        }
        copy = pltpu.make_async_remote_copy(
            src_ref=parts.at[0],
            dst_ref=parts.at[step],
            send_sem=part_send.at[step],
            recv_sem=part_recv.at[step],
            device_id=target,
            device_id_type=MESH,
        )
        copy.start()
        copies.append(copy)
    with jax.named_scope("drain"):
        for r in range(CHUNKS):
            to_x(r).wait_send()
            to_y(r).wait_send()
            to_core(r).wait_send()
            for slot in (2, 4, 6):
                share(r, slot).wait_send()
        for r in head:
            onward_y(r).wait_send()
            relay_x(r).wait_send()
    with jax.named_scope("exch"):
        for copy in copies:
            copy.wait_recv()
    total = jnp.sum(parts[...], axis=0)
    first = (qpoint * count_freq + freq) * OUT_DEV
    lanes = lax.broadcasted_iota(jnp.int32, total.shape, 1)
    spots = lax.broadcasted_iota(jnp.int32, (2, OUT_DEV), 1)
    result = jnp.zeros((2, OUT_DEV), jnp.float32)
    for j in range(OUT_DEV):
        picked = jnp.sum(jnp.where(lanes == first + j, total, 0.0), axis=1, keepdims=True)
        result = jnp.where(spots == j, picked, result)
    out_ref[...] = result.reshape(out_ref.shape)
    with jax.named_scope("sent"):
        for copy in copies:
            copy.wait_send()


def fused_body(densities, screened, energies, occupied, kmq, offsets, weights):
    count_pb = lax.axis_size("pb")
    count_freq = lax.axis_size("freq")
    count_ga = lax.axis_size("ga")
    pair_rows, basis = densities.shape[2:]
    panel_rows = screened.shape[3]
    group = count_freq * count_ga
    width = basis // CHUNKS
    cols = basis // PANELS
    total_out = OUT_DEV * count_pb * count_freq
    shape = (count_pb, count_freq, count_ga)
    anywhere = pl.BlockSpec(memory_space=pltpu.HBM)
    vector = pl.BlockSpec(memory_space=pltpu.VMEM)
    return pl.pallas_call(
        functools.partial(fused_kernel, shape),
        out_shape=jax.ShapeDtypeStruct((2, NS, OUT_DEV), jnp.float32),
        in_specs=[anywhere] * 7,
        out_specs=vector,
        scratch_shapes=[
            pltpu.VMEM((CHUNKS, SLOTS, 2, pair_rows, width), jnp.bfloat16),
            pltpu.VMEM((HALF, SLOTS, pair_rows, width), jnp.bfloat16),
            pltpu.VMEM((PANELS, 2, panel_rows, cols), jnp.bfloat16),
            pltpu.VMEM((PANELS, 8 * pair_rows, cols), jnp.float32),
            pltpu.VMEM((2, SLOTS, pair_rows, 128), jnp.float32),
            pltpu.VMEM((2, NB, total_out), jnp.float32),
            pltpu.VMEM((count_pb * group, 2, total_out), jnp.float32),
            pltpu.VMEM(energies.shape, energies.dtype),
            pltpu.SMEM(occupied.shape, occupied.dtype),
            pltpu.SMEM(kmq.shape, kmq.dtype),
            pltpu.SMEM(offsets.shape, offsets.dtype),
            pltpu.SMEM(weights.shape, weights.dtype),
            pltpu.SemaphoreType.DMA((CHUNKS,)),
            pltpu.SemaphoreType.DMA((PANELS,)),
            pltpu.SemaphoreType.DMA((5,)),
            pltpu.SemaphoreType.DMA((7, CHUNKS)),
            pltpu.SemaphoreType.DMA((CHUNKS, SLOTS)),
            pltpu.SemaphoreType.DMA((count_pb * group,)),
            pltpu.SemaphoreType.DMA((count_pb * group,)),
            pltpu.SemaphoreType.REGULAR((count_pb - 1,)),
        ],
        compiler_params=pltpu.CompilerParams(
            collective_id=0, has_side_effects=True, vmem_limit_bytes=46 * 2**20
        ),
    )(
        *(
            pltpu.with_memory_space_constraint(operand, pltpu.HBM)
            for operand in (densities, screened, energies, occupied, kmq, offsets, weights)
        )
    )


def body(densities, screened, *rest):
    basis, panel_rows = densities.shape[3], screened.shape[3]
    chips = lax.axis_size("freq") == 4 and lax.axis_size("ga") == 2 and lax.axis_size("pb") > 1
    fits = densities.shape[2] % 16 == 0 and basis % (PANELS * 128) == 0 and panel_rows * 2 == basis
    if chips and fits:
        return fused_body(densities, screened, *rest)
    return plain_body(densities, screened, *rest)


def solution(mesh):
    placed = (
        P("pb", None, ("freq", "ga"), None),
        P("pb", "freq", None, "ga", None),
        P(),
        P(),
        P(),
        P(),
        P(),
    )
    return jax.shard_map(
        body, mesh=mesh, in_specs=placed, out_specs=P(None, None, ("pb", "freq")), check_vma=False
    )
```

```python
import functools
import math

import jax
import jax.numpy as jnp
from jax import lax
from jax.experimental import pallas as pl
from jax.experimental.pallas import tpu as pltpu
from jax.sharding import PartitionSpec as P

MESH = pl.DeviceIdType.MESH
CHUNKS = 4
PANELS = 8
HALF = CHUNKS // 2
SLOTS = 8

NB = 256
NS = 1
OUT_DEV = 4


broadening = 0.15


def from_behind(block, axis, distance):
    devices = range(lax.axis_size(axis))
    route = [((i - distance) % len(devices), i) for i in devices]
    return lax.ppermute(block, axis, route)


def green_parts(level_row, filled, freq_shift, omegas):
    bands = jnp.arange(level_row.shape[0], dtype=jnp.int32)
    pole_sign = jnp.where(bands < filled, -1.0, 1.0).astype(jnp.float32)
    real_part = omegas[None, :] - freq_shift - level_row[:, None]
    imag_part = broadening * pole_sign[:, None]
    denominator = real_part * real_part + imag_part * imag_part
    return (real_part / denominator, -imag_part / denominator)


def spectrum(pair_real, pair_imag, green_real, green_imag):
    exact = lax.Precision.HIGHEST
    real_out = jnp.dot(pair_real, green_real, precision=exact) - jnp.dot(
        pair_imag, green_imag, precision=exact
    )
    imag_out = jnp.dot(pair_real, green_imag, precision=exact) + jnp.dot(
        pair_imag, green_real, precision=exact
    )
    return jnp.stack([real_out, imag_out])


def panel_product(density_all, screen):
    pair_rows = density_all.shape[1]
    panel_rows = screen.shape[1]
    product = lax.dot_general(
        density_all.reshape(2 * pair_rows, -1),
        screen.reshape(2 * panel_rows, -1),
        (((1,), (1,)), ((), ())),
        preferred_element_type=jnp.float32,
    )
    product = product.reshape(2, pair_rows, 2, panel_rows)
    return (product[0, :, 0] - product[1, :, 1], product[0, :, 1] + product[1, :, 0])


def plain_body(densities, screened, energies, occupied, kmq, offsets, weights):
    qpoint = lax.axis_index("pb")
    my_freq = lax.axis_index("freq")
    my_panel = lax.axis_index("ga")
    count_pb = lax.axis_size("pb")
    count_freq = lax.axis_size("freq")
    screen = screened[0, 0]
    panel_width = screen.shape[1]
    local_block = densities[0]
    whole = lax.all_gather(local_block, ("freq", "ga"), axis=1, tiled=True)
    real_x, imag_x = panel_product(whole, screen)
    own_rows = lax.dynamic_slice_in_dim(whole, my_panel * panel_width, panel_width, 2)
    dense = own_rows.astype(jnp.float32)
    real_sum = jnp.sum(dense[0] * real_x + dense[1] * imag_x, axis=1)
    imag_sum = jnp.sum(dense[0] * imag_x - dense[1] * real_x, axis=1)
    pair_total = lax.psum(jnp.stack([real_sum, imag_sum]), "ga")
    weighted = (pair_total * weights[my_freq]).reshape(2, NS, NB)
    kpoint = kmq[qpoint]
    level_row = energies[kpoint]
    filled = occupied[kpoint]
    total_out = OUT_DEV * count_pb * count_freq
    index_grid = (jnp.arange(count_pb, dtype=jnp.int32)[:, None] * count_freq + my_freq) * OUT_DEV
    index_grid = (index_grid + jnp.arange(OUT_DEV, dtype=jnp.int32)[None, :]).reshape(-1)
    omegas = -2.0 + 4.0 * index_grid.astype(jnp.float32) / total_out
    summed = jnp.zeros((2, NS, count_pb * OUT_DEV), jnp.float32)
    passed = weighted
    for rotation in range(count_freq):
        anchor = (my_freq - rotation) % count_freq
        freq_shift = 4.0 * offsets[anchor].astype(jnp.float32) / total_out
        green_real, green_imag = green_parts(level_row, filled, freq_shift, omegas)
        summed = summed + spectrum(passed[0], passed[1], green_real, green_imag)
        if rotation + 1 < count_freq:
            passed = from_behind(passed, "freq", 1)
    local_part = lax.psum_scatter(summed, "pb", scatter_dimension=2, tiled=True)
    prefactor = 1.0 / (2.0 * math.pi * count_pb)
    return jnp.stack([-prefactor * local_part[1], prefactor * local_part[0]])


def fused_kernel(
    shape,
    dens_hbm,
    screen_hbm,
    energy_hbm,
    filled_hbm,
    kmq_hbm,
    offset_hbm,
    weight_hbm,
    out_ref,
    dens,
    minus,
    panel,
    acc,
    psum,
    green,
    parts,
    energy,
    filled,
    kmq,
    offset,
    weight,
    own_sem,
    panel_sem,
    small_sem,
    send_sem,
    recv_sem,
    core_sem,
    part_send,
    part_recv,
    ready,
):
    count_pb, count_freq, count_ga = shape
    group = count_freq * count_ga
    rows = dens.shape[3]
    width = dens.shape[4]
    cols = panel.shape[3]
    per = width // cols
    total_out = green.shape[2]
    qpoint = lax.axis_index("pb")
    freq = lax.axis_index("freq")
    x = lax.axis_index("ga")
    y, core = freq // 2, freq % 2
    ny, nx, nc = 1 - y, 1 - x, 1 - core
    at_x = {"freq": freq, "ga": nx}
    at_y = {"freq": ny * 2 + core, "ga": x}
    at_core = {"freq": y * 2 + nc, "ga": x}

    def place(yy, cc, xx):
        return (yy * 2 + cc) * count_ga + xx

    def owner(slot):
        dy, dx, dc = slot // 4, slot // 2 % 2, slot % 2
        return place((y + dy) % 2, (core + dc) % 2, (x + dx) % 2)

    barrier = pltpu.get_barrier_semaphore()
    for target in (at_x, at_y, at_core):
        pl.semaphore_signal(barrier, inc=1, device_id=target, device_id_type=MESH)

    def both_layers(semaphore):
        @pl.when(qpoint > 0)
        def _():
            pl.semaphore_signal(
                semaphore, inc=1, device_id={"pb": qpoint - 1}, device_id_type=MESH
            )

        @pl.when(qpoint < count_pb - 1)
        def _():
            pl.semaphore_signal(
                semaphore, inc=1, device_id={"pb": qpoint + 1}, device_id_type=MESH
            )

    layers = (qpoint + count_pb - 1) // count_pb + (2 * count_pb - 2 - qpoint) // count_pb
    both_layers(barrier)

    def own_copy(r):
        start = pl.multiple_of((x * HALF + r) % CHUNKS * width, width)
        return pltpu.make_async_copy(
            dens_hbm.at[0, :, :, pl.ds(start, width)], dens.at[r, 0], own_sem
        )

    def panel_copy(n):
        start = pl.multiple_of((x * (PANELS // 2) + n) % PANELS * cols, cols)
        return pltpu.make_async_copy(
            screen_hbm.at[0, 0, :, :, pl.ds(start, cols)], panel.at[n], panel_sem.at[n]
        )

    first_own = [HALF + r for r in range(HALF)] + list(range(HALF))
    for r in range(CHUNKS):
        own_copy(r).start()
    small = [
        pltpu.make_async_copy(source, target, small_sem.at[i])
        for i, (source, target) in enumerate(
            [
                (energy_hbm, energy),
                (filled_hbm, filled),
                (kmq_hbm, kmq),
                (offset_hbm, offset),
                (weight_hbm, weight),
            ]
        )
    ]
    for copy in small:
        copy.start()
    for n in range(PANELS):
        panel_copy(n).start(priority=1)

    pairs = [((0, 2), (0, 4)), ((0, 3), (0, 5)), ((1, 2), (1, 4)), ((1, 3), (1, 5))]
    pairs += [((2, 2), (0, 6)), ((3, 2), (1, 6)), ((2, 3), (3, 3)), ((2, 4), (2, 6))]
    pairs += [((3, 4), (3, 6)), ((2, 5), (2, 7)), ((3, 5), (3, 7)), ((0, 7),), ((1, 7),)]
    numbers = {block: i for i, pair in enumerate(pairs) for block in pair}

    def remote(r, slot, there, slot_there, target, group_of):
        return pltpu.make_async_remote_copy(
            src_ref=dens.at[r, slot],
            dst_ref=dens.at[there, slot_there],
            send_sem=send_sem.at[group_of],
            recv_sem=recv_sem.at[numbers[there, slot_there]],
            device_id=target,
            device_id_type=MESH,
        )

    def to_x(r):
        return remote(r, 0, (r + HALF) % CHUNKS, 2, at_x, r)

    def to_y(r):
        return remote(r, 0, r, 4, at_y, r)

    def to_core(r):
        return pltpu.make_async_remote_copy(
            src_ref=dens.at[r, 0],
            dst_ref=dens.at[r, 1],
            send_sem=send_sem.at[r],
            recv_sem=core_sem,
            device_id=at_core,
            device_id_type=MESH,
        )

    def siblings():
        return pltpu.make_async_remote_copy(
            src_ref=dens.at[:, 1],
            dst_ref=dens.at[:, 1],
            send_sem=send_sem.at[0],
            recv_sem=core_sem,
            device_id=at_core,
            device_id_type=MESH,
        )

    def onward_y(r):
        return remote(r, 2, r, 6, at_y, r)

    def relay_x(r):
        return remote(r, 4, r + HALF, 6, at_x, r + HALF)

    def share(r, slot):
        return remote(r, slot, r, slot + 1, at_core, r)

    def all_sent(r):
        pltpu.make_async_remote_copy(
            src_ref=dens.at[r, 1:],
            dst_ref=dens.at[r, 1:],
            send_sem=send_sem.at[r],
            recv_sem=core_sem,
            device_id=at_core,
            device_id_type=MESH,
        ).wait_send()

    def arrived(*blocks):
        number = pairs.index(blocks)
        landed = dens.at[0, 1 : 1 + len(blocks)]
        pltpu.make_async_remote_copy(
            src_ref=landed,
            dst_ref=landed,
            send_sem=send_sem.at[0],
            recv_sem=recv_sem.at[number],
            device_id=at_core,
            device_id_type=MESH,
        ).wait_recv()

    def take(*blocks):
        arrived(*blocks)
        for r, slot in blocks:
            share(r, slot).start()

    def pass_ready(step):
        if step < count_pb - 1:
            pl.semaphore_wait(ready.at[step - 1], layers)
            both_layers(ready.at[step])

    def prepare(r, slots):
        for slot in slots:
            minus[r, slot] = -dens[r, slot, 1]

    with jax.named_scope("bar"):
        pl.semaphore_wait(barrier, 3 + layers)
    with jax.named_scope("own"):
        pltpu.make_async_copy(dens.at[:, 0], dens.at[:, 0], own_sem).wait()
    for r in first_own:
        if r >= HALF:
            to_x(r).start()
        else:
            to_y(r).start()
        to_core(r).start()
    for r in range(HALF):
        to_x(r).start()

    with jax.named_scope("small"):
        for copy in small:
            copy.wait()
    kpoint = kmq[qpoint]
    level_row = energy[pl.ds(kpoint, 1), :]
    levels = jnp.broadcast_to(level_row, (8, level_row.shape[1])).T[:, :1]
    bands = lax.broadcasted_iota(jnp.int32, (level_row.shape[1], total_out), 0)
    grid = lax.broadcasted_iota(jnp.int32, (level_row.shape[1], total_out), 1)
    omegas = -2.0 + 4.0 * grid.astype(jnp.float32) / total_out
    freq_shift = 4.0 * offset[freq].astype(jnp.float32) / total_out
    real_part = omegas - freq_shift - levels
    imag_part = jnp.where(bands < filled[kpoint], -broadening, broadening)
    scale = weight[freq] / (2.0 * math.pi * count_pb)
    inverse = scale / (real_part * real_part + imag_part * imag_part)
    green[0] = real_part * inverse
    green[1] = -imag_part * inverse

    def product(slots, chunks, n):
        low = chunks[0] * width
        depth = len(chunks) * width
        left = []
        for plane in range(2):
            for r in chunks:
                pieces = []
                for slot in slots:
                    if plane == 0:
                        pieces += [dens[r, slot, 0], minus[r, slot]]
                    else:
                        pieces += [dens[r, slot, 1], dens[r, slot, 0]]
                left.append(jnp.concatenate(pieces, axis=0))
        right = [panel[n, plane, low : low + depth, :] for plane in range(2)]
        return lax.dot_general(
            jnp.concatenate(left, axis=1),
            jnp.concatenate(right, axis=0),
            (((1,), (0,)), ((), ())),
            preferred_element_type=jnp.float32,
        )

    started = set()

    def spectra(slots):
        real_out = jnp.zeros((rows, total_out), jnp.float32)
        imag_out = jnp.zeros((rows, total_out), jnp.float32)
        for slot in slots:
            pair_real = jnp.sum(psum[0, slot], axis=1, keepdims=True)
            pair_imag = jnp.sum(psum[1, slot], axis=1, keepdims=True)
            here = pl.ds(pl.multiple_of(owner(slot) * rows, rows), rows)
            green_real, green_imag = green[0, here, :], green[1, here, :]
            real_out = real_out + pair_real * green_real - pair_imag * green_imag
            imag_out = imag_out + pair_real * green_imag + pair_imag * green_real
        return real_out, imag_out

    head = list(range(HALF))
    half = PANELS // 2

    def parts_of(value, slots):
        return [(slot, value[2 * i * rows : 2 * (i + 1) * rows]) for i, slot in enumerate(slots)]

    def first_part(slots, n):
        for slot, value in parts_of(product(slots, [0], n), slots):
            acc[n, slot] = value

    def last_part(slots, n):
        for slot, value in parts_of(product(slots, [1], n), slots):
            acc[n, slot] += value

    def settle(slots, n):
        r, off = n // per, n % per * cols
        for slot in slots:
            real_y, imag_y = acc[n, slot, :rows], acc[n, slot, rows:]
            real_d = dens[r, slot, 0, :, off : off + cols].astype(jnp.float32)
            imag_d = dens[r, slot, 1, :, off : off + cols].astype(jnp.float32)
            real = real_y * real_d - imag_y * imag_d
            imag = real_y * imag_d + imag_y * real_d
            for c, total in enumerate((real, imag)):
                narrow = total[:, :128]
                for part in range(1, cols // 128):
                    narrow = narrow + total[:, part * 128 : (part + 1) * 128]
                if slot in started:
                    psum[c, slot] += narrow
                else:
                    psum[c, slot] = narrow
            started.add(slot)

    def own_block(n):
        with jax.named_scope(f"pan{n}"):
            panel_copy(n).wait()
        for slot, value in parts_of(product(own, head, n), own):
            acc[n, slot] = value

    own, xs, ys, far = (0, 1), (2, 3), (4, 5), (6, 7)
    near, direct, shared = xs + ys, (2, 4), (3, 5)
    for r in head:
        prepare(r, (0,))
    with jax.named_scope("sib"):
        siblings().wait_recv()
    for r in head:
        prepare(r, (1,))
    def finish(products, settled):
        done = 0
        for i, (slots, n) in enumerate(products):
            last_part(slots, n)
            until = len(settled) * (i + 1) // len(products)
            for pair, m in settled[done:until]:
                settle(pair, m)
            done = until

    own_block(0)
    for n in range(1, half):
        own_block(n)
        settle(own, n - 1)
    with jax.named_scope("take0"):
        take((0, 2), (0, 4))
        onward_y(0).start()
        relay_x(0).start()
    prepare(0, direct)
    for n in range(3):
        first_part(direct, n)
    settle(own, 3)
    own_block(4)
    with jax.named_scope("got0"):
        arrived((0, 3), (0, 5))
    prepare(0, shared)
    first_part(shared, 0)
    settle(own, 4)
    first_part(shared, 1)
    first_part(shared, 2)
    first_part(near, 3)
    with jax.named_scope("take1"):
        take((1, 2), (1, 4))
        onward_y(1).start()
        relay_x(1).start()
        for r in range(HALF, CHUNKS):
            to_y(r).start()
        panel_copy(5).wait()
        panel_copy(6).wait()
    first_part(near, 4)
    first_part(own + near, 5)
    first_part(own + near, 6)
    prepare(1, direct)
    last_part(direct, 0)
    last_part(direct, 1)
    with jax.named_scope("take2"):
        take((2, 2), (0, 6))
        arrived((1, 3), (1, 5))
        panel_copy(7).wait()
    first_part(own + near, 7)
    prepare(1, shared)
    last_part(shared, 0)
    last_part(shared, 1)
    steps = [(pair, n) for n in range(5) for pair in (xs, ys)]
    finish(steps[4:], steps[:8])
    with jax.named_scope("take3"):
        take((3, 2), (1, 6))
        arrived((0, 7),)
        both_layers(ready.at[0])
    prepare(0, far)
    for n in range(PANELS):
        first_part(far, n)
    with jax.named_scope("take4"):
        take((2, 4), (2, 6))
        arrived((1, 7),)
        arrived((2, 3), (3, 3))
    prepare(1, far)
    steps = [(far, n) for n in range(PANELS)]
    finish(steps[:1], [])
    finish(steps[1:], [(xs, 4)] + steps[:4])
    with jax.named_scope("take5"):
        arrived((2, 5), (2, 7))
        take((3, 4), (3, 6))
        pass_ready(1)
    steps = [(pair, n) for n in (5, 6) for pair in (own, xs, ys)]
    finish(steps[:1], [(ys, 4)])
    finish(steps[1:], [(far, 4), steps[0], (far, 5), steps[1], steps[2], steps[3]])
    with jax.named_scope("last3"):
        arrived((3, 5), (3, 7))
        for step in range(2, count_pb - 1):
            pass_ready(step)
    finish([(own, 7), (xs, 7)], [(xs, 6), (ys, 6), (own, 7), (far, 6)])
    finish([(ys, 7)], [(far, 7), (xs, 7)])
    early = spectra((0, 1, 2, 3, 6, 7))
    settle(ys, 7)
    late = spectra((4, 5))
    parts[0, 0:1] = -jnp.sum(early[1] + late[1], axis=0, keepdims=True)
    parts[0, 1:2] = jnp.sum(early[0] + late[0], axis=0, keepdims=True)
    with jax.named_scope("ready"):
        pl.semaphore_wait(ready.at[count_pb - 2], layers)
    me = owner(0)
    down = qpoint < count_pb // 2
    for turn in range(count_pb):
        if turn < count_pb - 1:
            high, low = count_pb - 1 - turn, turn
            high = jnp.where(high > qpoint, high, high - 1)
            low = jnp.where(low < qpoint, low, low + 1)
            layer = jnp.where(down, high, low)
        else:
            layer = qpoint
        turned = (layer + count_pb - qpoint) % count_pb * group
        for step in range(group - 1, -1, -1):
            if turn == count_pb - 1 and step == 0:
                continue
            spot = (me + step) % group
            pltpu.make_async_remote_copy(
                src_ref=parts.at[0],
                dst_ref=parts.at[turned + step],
                send_sem=part_send,
                recv_sem=part_recv,
                device_id={"pb": layer, "freq": spot // count_ga, "ga": spot % count_ga},
                device_id_type=MESH,
            ).start()
    with jax.named_scope("drain"):
        for r in range(CHUNKS):
            all_sent(r)
    others = pltpu.make_async_remote_copy(
        src_ref=parts.at[1:],
        dst_ref=parts.at[1:],
        send_sem=part_send,
        recv_sem=part_recv,
        device_id=at_core,
        device_id_type=MESH,
    )
    with jax.named_scope("exch"):
        others.wait_recv()
    total = jnp.sum(parts[...], axis=0)
    first = (qpoint * count_freq + freq) * OUT_DEV
    lanes = lax.broadcasted_iota(jnp.int32, total.shape, 1)
    spots = lax.broadcasted_iota(jnp.int32, (2, OUT_DEV), 1)
    result = jnp.zeros((2, OUT_DEV), jnp.float32)
    for j in range(OUT_DEV):
        picked = jnp.sum(jnp.where(lanes == first + j, total, 0.0), axis=1, keepdims=True)
        result = jnp.where(spots == j, picked, result)
    out_ref[...] = result.reshape(out_ref.shape)
    with jax.named_scope("sent"):
        others.wait_send()


def fused_body(densities, screened, energies, occupied, kmq, offsets, weights):
    count_pb = lax.axis_size("pb")
    count_freq = lax.axis_size("freq")
    count_ga = lax.axis_size("ga")
    pair_rows, basis = densities.shape[2:]
    panel_rows = screened.shape[3]
    group = count_freq * count_ga
    width = basis // CHUNKS
    cols = basis // PANELS
    total_out = OUT_DEV * count_pb * count_freq
    shape = (count_pb, count_freq, count_ga)
    anywhere = pl.BlockSpec(memory_space=pltpu.HBM)
    vector = pl.BlockSpec(memory_space=pltpu.VMEM)
    return pl.pallas_call(
        functools.partial(fused_kernel, shape),
        out_shape=jax.ShapeDtypeStruct((2, NS, OUT_DEV), jnp.float32),
        in_specs=[anywhere] * 7,
        out_specs=vector,
        scratch_shapes=[
            pltpu.VMEM((CHUNKS, SLOTS, 2, pair_rows, width), jnp.bfloat16),
            pltpu.VMEM((HALF, SLOTS, pair_rows, width), jnp.bfloat16),
            pltpu.VMEM((PANELS, 2, panel_rows, cols), jnp.bfloat16),
            pltpu.VMEM((PANELS, SLOTS, 2 * pair_rows, cols), jnp.float32),
            pltpu.VMEM((2, SLOTS, pair_rows, 128), jnp.float32),
            pltpu.VMEM((2, NB, total_out), jnp.float32),
            pltpu.VMEM((count_pb * group, 2, total_out), jnp.float32),
            pltpu.VMEM(energies.shape, energies.dtype),
            pltpu.SMEM(occupied.shape, occupied.dtype),
            pltpu.SMEM(kmq.shape, kmq.dtype),
            pltpu.SMEM(offsets.shape, offsets.dtype),
            pltpu.SMEM(weights.shape, weights.dtype),
            pltpu.SemaphoreType.DMA,
            pltpu.SemaphoreType.DMA((PANELS,)),
            pltpu.SemaphoreType.DMA((5,)),
            pltpu.SemaphoreType.DMA((CHUNKS,)),
            pltpu.SemaphoreType.DMA((13,)),
            pltpu.SemaphoreType.DMA,
            pltpu.SemaphoreType.DMA,
            pltpu.SemaphoreType.DMA,
            pltpu.SemaphoreType.REGULAR((count_pb - 1,)),
        ],
        compiler_params=pltpu.CompilerParams(
            collective_id=0, has_side_effects=True, vmem_limit_bytes=50 * 2**20
        ),
    )(
        *(
            pltpu.with_memory_space_constraint(operand, pltpu.HBM)
            for operand in (densities, screened, energies, occupied, kmq, offsets, weights)
        )
    )


def body(densities, screened, *rest):
    basis, panel_rows = densities.shape[3], screened.shape[3]
    chips = lax.axis_size("freq") == 4 and lax.axis_size("ga") == 2 and lax.axis_size("pb") > 1
    fits = densities.shape[2] % 16 == 0 and basis % (PANELS * 128) == 0 and panel_rows * 2 == basis
    if chips and fits:
        return fused_body(densities, screened, *rest)
    return plain_body(densities, screened, *rest)


def solution(mesh):
    placed = (
        P("pb", None, ("freq", "ga"), None),
        P("pb", "freq", None, "ga", None),
        P(),
        P(),
        P(),
        P(),
        P(),
    )
    return jax.shard_map(
        body, mesh=mesh, in_specs=placed, out_specs=P(None, None, ("pb", "freq")), check_vma=False
    )
```

```python
import functools
import math

import jax
import jax.numpy as jnp
from jax import lax
from jax.experimental import pallas as pl
from jax.experimental.pallas import tpu as pltpu
from jax.sharding import PartitionSpec as P

MESH = pl.DeviceIdType.MESH
CHUNKS = 4
PANELS = 8
HALF = CHUNKS // 2
SLOTS = 8

NB = 256
NS = 1
OUT_DEV = 4


broadening = 0.15


def from_behind(block, axis, distance):
    devices = range(lax.axis_size(axis))
    route = [((i - distance) % len(devices), i) for i in devices]
    return lax.ppermute(block, axis, route)


def green_parts(level_row, filled, freq_shift, omegas):
    bands = jnp.arange(level_row.shape[0], dtype=jnp.int32)
    pole_sign = jnp.where(bands < filled, -1.0, 1.0).astype(jnp.float32)
    real_part = omegas[None, :] - freq_shift - level_row[:, None]
    imag_part = broadening * pole_sign[:, None]
    denominator = real_part * real_part + imag_part * imag_part
    return (real_part / denominator, -imag_part / denominator)


def spectrum(pair_real, pair_imag, green_real, green_imag):
    exact = lax.Precision.HIGHEST
    real_out = jnp.dot(pair_real, green_real, precision=exact) - jnp.dot(
        pair_imag, green_imag, precision=exact
    )
    imag_out = jnp.dot(pair_real, green_imag, precision=exact) + jnp.dot(
        pair_imag, green_real, precision=exact
    )
    return jnp.stack([real_out, imag_out])


def panel_product(density_all, screen):
    pair_rows = density_all.shape[1]
    panel_rows = screen.shape[1]
    product = lax.dot_general(
        density_all.reshape(2 * pair_rows, -1),
        screen.reshape(2 * panel_rows, -1),
        (((1,), (1,)), ((), ())),
        preferred_element_type=jnp.float32,
    )
    product = product.reshape(2, pair_rows, 2, panel_rows)
    return (product[0, :, 0] - product[1, :, 1], product[0, :, 1] + product[1, :, 0])


def plain_body(densities, screened, energies, occupied, kmq, offsets, weights):
    qpoint = lax.axis_index("pb")
    my_freq = lax.axis_index("freq")
    my_panel = lax.axis_index("ga")
    count_pb = lax.axis_size("pb")
    count_freq = lax.axis_size("freq")
    screen = screened[0, 0]
    panel_width = screen.shape[1]
    local_block = densities[0]
    whole = lax.all_gather(local_block, ("freq", "ga"), axis=1, tiled=True)
    real_x, imag_x = panel_product(whole, screen)
    own_rows = lax.dynamic_slice_in_dim(whole, my_panel * panel_width, panel_width, 2)
    dense = own_rows.astype(jnp.float32)
    real_sum = jnp.sum(dense[0] * real_x + dense[1] * imag_x, axis=1)
    imag_sum = jnp.sum(dense[0] * imag_x - dense[1] * real_x, axis=1)
    pair_total = lax.psum(jnp.stack([real_sum, imag_sum]), "ga")
    weighted = (pair_total * weights[my_freq]).reshape(2, NS, NB)
    kpoint = kmq[qpoint]
    level_row = energies[kpoint]
    filled = occupied[kpoint]
    total_out = OUT_DEV * count_pb * count_freq
    index_grid = (jnp.arange(count_pb, dtype=jnp.int32)[:, None] * count_freq + my_freq) * OUT_DEV
    index_grid = (index_grid + jnp.arange(OUT_DEV, dtype=jnp.int32)[None, :]).reshape(-1)
    omegas = -2.0 + 4.0 * index_grid.astype(jnp.float32) / total_out
    summed = jnp.zeros((2, NS, count_pb * OUT_DEV), jnp.float32)
    passed = weighted
    for rotation in range(count_freq):
        anchor = (my_freq - rotation) % count_freq
        freq_shift = 4.0 * offsets[anchor].astype(jnp.float32) / total_out
        green_real, green_imag = green_parts(level_row, filled, freq_shift, omegas)
        summed = summed + spectrum(passed[0], passed[1], green_real, green_imag)
        if rotation + 1 < count_freq:
            passed = from_behind(passed, "freq", 1)
    local_part = lax.psum_scatter(summed, "pb", scatter_dimension=2, tiled=True)
    prefactor = 1.0 / (2.0 * math.pi * count_pb)
    return jnp.stack([-prefactor * local_part[1], prefactor * local_part[0]])


def fused_kernel(
    shape,
    dens_hbm,
    screen_hbm,
    energy_hbm,
    filled_hbm,
    kmq_hbm,
    offset_hbm,
    weight_hbm,
    out_ref,
    dens,
    minus,
    panel,
    acc,
    psum,
    green,
    parts,
    energy,
    filled,
    kmq,
    offset,
    weight,
    own_sem,
    panel_sem,
    small_sem,
    send_sem,
    recv_sem,
    core_sem,
    part_send,
    part_recv,
    ready,
):
    count_pb, count_freq, count_ga = shape
    group = count_freq * count_ga
    rows = dens.shape[3]
    width = dens.shape[4]
    cols = panel.shape[3]
    per = width // cols
    total_out = green.shape[2]
    qpoint = lax.axis_index("pb")
    freq = lax.axis_index("freq")
    x = lax.axis_index("ga")
    y, core = freq // 2, freq % 2
    ny, nx, nc = 1 - y, 1 - x, 1 - core
    at_x = {"freq": freq, "ga": nx}
    at_y = {"freq": ny * 2 + core, "ga": x}
    at_core = {"freq": y * 2 + nc, "ga": x}

    def place(yy, cc, xx):
        return (yy * 2 + cc) * count_ga + xx

    def owner(slot):
        dy, dx, dc = slot // 4, slot // 2 % 2, slot % 2
        return place((y + dy) % 2, (core + dc) % 2, (x + dx) % 2)

    barrier = pltpu.get_barrier_semaphore()
    for target in (at_x, at_y, at_core):
        pl.semaphore_signal(barrier, inc=1, device_id=target, device_id_type=MESH)

    def both_layers(semaphore):
        @pl.when(qpoint > 0)
        def _():
            pl.semaphore_signal(
                semaphore, inc=1, device_id={"pb": qpoint - 1}, device_id_type=MESH
            )

        @pl.when(qpoint < count_pb - 1)
        def _():
            pl.semaphore_signal(
                semaphore, inc=1, device_id={"pb": qpoint + 1}, device_id_type=MESH
            )

    layers = (qpoint + count_pb - 1) // count_pb + (2 * count_pb - 2 - qpoint) // count_pb
    both_layers(barrier)

    def own_copy(r):
        start = pl.multiple_of((x * HALF + r) % CHUNKS * width, width)
        return pltpu.make_async_copy(
            dens_hbm.at[0, :, :, pl.ds(start, width)], dens.at[r, 0], own_sem
        )

    def panel_copy(n):
        start = pl.multiple_of((x * (PANELS // 2) + n) % PANELS * cols, cols)
        return pltpu.make_async_copy(
            screen_hbm.at[0, 0, :, :, pl.ds(start, cols)], panel.at[n], panel_sem.at[n]
        )

    for r in range(CHUNKS):
        own_copy(r).start()
    small = [
        pltpu.make_async_copy(source, target, small_sem.at[i])
        for i, (source, target) in enumerate(
            [
                (energy_hbm, energy),
                (filled_hbm, filled),
                (kmq_hbm, kmq),
                (offset_hbm, offset),
                (weight_hbm, weight),
            ]
        )
    ]
    for copy in small:
        copy.start()
    for n in range(PANELS):
        panel_copy(n).start(priority=1)

    pairs = [((0, 2), (0, 4)), ((0, 3), (0, 5)), ((1, 2), (1, 4)), ((1, 3), (1, 5))]
    pairs += [((2, 2), (0, 6)), ((3, 2), (1, 6)), ((2, 3), (3, 3)), ((2, 4), (2, 6))]
    pairs += [((3, 4), (3, 6)), ((2, 5), (2, 7)), ((3, 5), (3, 7)), ((0, 7),), ((1, 7),)]
    numbers = {block: i for i, pair in enumerate(pairs) for block in pair}

    cuts = [slice(0, width // 2), slice(width // 2, width)]

    def remote(r, slot, there, slot_there, target, group_of, cut=slice(None)):
        number = numbers[there, slot_there]
        if (there, slot_there) in pairs[0] and cut == cuts[0]:
            number = len(pairs)
        return pltpu.make_async_remote_copy(
            src_ref=dens.at[r, slot, :, :, cut],
            dst_ref=dens.at[there, slot_there, :, :, cut],
            send_sem=send_sem.at[group_of],
            recv_sem=recv_sem.at[number],
            device_id=target,
            device_id_type=MESH,
        )

    def to_x(r, cut=slice(None)):
        return remote(r, 0, (r + HALF) % CHUNKS, 2, at_x, r, cut)

    def to_y(r, cut=slice(None)):
        return remote(r, 0, r, 4, at_y, r, cut)

    def to_core(r):
        return pltpu.make_async_remote_copy(
            src_ref=dens.at[r, 0],
            dst_ref=dens.at[r, 1],
            send_sem=send_sem.at[r],
            recv_sem=core_sem,
            device_id=at_core,
            device_id_type=MESH,
        )

    def siblings():
        return pltpu.make_async_remote_copy(
            src_ref=dens.at[:, 1],
            dst_ref=dens.at[:, 1],
            send_sem=send_sem.at[0],
            recv_sem=core_sem,
            device_id=at_core,
            device_id_type=MESH,
        )

    def onward_y(r):
        return remote(r, 2, r, 6, at_y, r)

    def relay_x(r):
        return remote(r, 4, r + HALF, 6, at_x, r + HALF)

    def share(r, slot, cut=slice(None)):
        return remote(r, slot, r, slot + 1, at_core, r, cut)

    def all_sent(r):
        pltpu.make_async_remote_copy(
            src_ref=dens.at[r, 1:],
            dst_ref=dens.at[r, 1:],
            send_sem=send_sem.at[r],
            recv_sem=core_sem,
            device_id=at_core,
            device_id_type=MESH,
        ).wait_send()

    def arrived(*blocks):
        number = pairs.index(blocks)
        landed = dens.at[0, 1 : 1 + len(blocks)]
        pltpu.make_async_remote_copy(
            src_ref=landed,
            dst_ref=landed,
            send_sem=send_sem.at[0],
            recv_sem=recv_sem.at[number],
            device_id=at_core,
            device_id_type=MESH,
        ).wait_recv()

    def take_piece(piece):
        landed = dens.at[0, 1]
        pltpu.make_async_remote_copy(
            src_ref=landed,
            dst_ref=landed,
            send_sem=send_sem.at[0],
            recv_sem=recv_sem.at[0 if piece else len(pairs)],
            device_id=at_core,
            device_id_type=MESH,
        ).wait_recv()
        for r, slot in pairs[0]:
            share(r, slot, cuts[piece]).start()

    def take(*blocks):
        arrived(*blocks)
        for r, slot in blocks:
            share(r, slot).start()

    def pass_ready(step):
        if step < count_pb - 1:
            pl.semaphore_wait(ready.at[step - 1], layers)
            both_layers(ready.at[step])

    def prepare(r, slots, cut=slice(None)):
        for slot in slots:
            minus[r, slot, :, cut] = -dens[r, slot, 1, :, cut]

    with jax.named_scope("bar"):
        pl.semaphore_wait(barrier, 3 + layers)
    with jax.named_scope("own"):
        pltpu.make_async_copy(dens.at[:, 0], dens.at[:, 0], own_sem).wait()
    for cut in cuts:
        to_x(HALF, cut).start()
        to_y(0, cut).start()
    for r in range(CHUNKS):
        to_core(r).start()
    for r in range(1, HALF):
        to_x(HALF + r).start()
        to_y(r).start()
    for r in range(HALF):
        to_x(r).start()

    with jax.named_scope("small"):
        for copy in small:
            copy.wait()
    kpoint = kmq[qpoint]
    level_row = energy[pl.ds(kpoint, 1), :]
    levels = jnp.broadcast_to(level_row, (8, level_row.shape[1])).T[:, :1]
    bands = lax.broadcasted_iota(jnp.int32, (level_row.shape[1], total_out), 0)
    grid = lax.broadcasted_iota(jnp.int32, (level_row.shape[1], total_out), 1)
    omegas = -2.0 + 4.0 * grid.astype(jnp.float32) / total_out
    freq_shift = 4.0 * offset[freq].astype(jnp.float32) / total_out
    real_part = omegas - freq_shift - levels
    imag_part = jnp.where(bands < filled[kpoint], -broadening, broadening)
    scale = weight[freq] / (2.0 * math.pi * count_pb)
    inverse = scale / (real_part * real_part + imag_part * imag_part)
    green[0] = real_part * inverse
    green[1] = -imag_part * inverse

    def product(slots, chunks, n, cut=slice(None)):
        low = chunks[0] * width + (cut.start or 0)
        depth = (cut.stop - cut.start) if cut.stop else len(chunks) * width
        left = []
        for plane in range(2):
            for r in chunks:
                pieces = []
                for slot in slots:
                    if plane == 0:
                        pieces += [dens[r, slot, 0, :, cut], minus[r, slot, :, cut]]
                    else:
                        pieces += [dens[r, slot, 1, :, cut], dens[r, slot, 0, :, cut]]
                left.append(jnp.concatenate(pieces, axis=0))
        right = [panel[n, plane, low : low + depth, :] for plane in range(2)]
        return lax.dot_general(
            jnp.concatenate(left, axis=1),
            jnp.concatenate(right, axis=0),
            (((1,), (0,)), ((), ())),
            preferred_element_type=jnp.float32,
        )

    started = set()

    def spectra(slots):
        real_out = jnp.zeros((rows, total_out), jnp.float32)
        imag_out = jnp.zeros((rows, total_out), jnp.float32)
        for slot in slots:
            pair_real = jnp.sum(psum[0, slot], axis=1, keepdims=True)
            pair_imag = jnp.sum(psum[1, slot], axis=1, keepdims=True)
            here = pl.ds(pl.multiple_of(owner(slot) * rows, rows), rows)
            green_real, green_imag = green[0, here, :], green[1, here, :]
            real_out = real_out + pair_real * green_real - pair_imag * green_imag
            imag_out = imag_out + pair_real * green_imag + pair_imag * green_real
        return real_out, imag_out

    head = list(range(HALF))
    half = PANELS // 2

    def parts_of(value, slots):
        return [(slot, value[2 * i * rows : 2 * (i + 1) * rows]) for i, slot in enumerate(slots)]

    def first_part(slots, n, cut=slice(None)):
        for slot, value in parts_of(product(slots, [0], n, cut), slots):
            if cut.start:
                acc[n, slot] += value
            else:
                acc[n, slot] = value

    def last_part(slots, n):
        for slot, value in parts_of(product(slots, [1], n), slots):
            acc[n, slot] += value

    def settle(slots, n):
        r, off = n // per, n % per * cols
        for slot in slots:
            real_y, imag_y = acc[n, slot, :rows], acc[n, slot, rows:]
            real_d = dens[r, slot, 0, :, off : off + cols].astype(jnp.float32)
            imag_d = dens[r, slot, 1, :, off : off + cols].astype(jnp.float32)
            real = real_y * real_d - imag_y * imag_d
            imag = real_y * imag_d + imag_y * real_d
            for c, total in enumerate((real, imag)):
                narrow = total[:, :128]
                for part in range(1, cols // 128):
                    narrow = narrow + total[:, part * 128 : (part + 1) * 128]
                if slot in started:
                    psum[c, slot] += narrow
                else:
                    psum[c, slot] = narrow
            started.add(slot)

    def own_block(n):
        with jax.named_scope(f"pan{n}"):
            panel_copy(n).wait()
        for slot, value in parts_of(product(own, head, n), own):
            acc[n, slot] = value

    own, xs, ys, far = (0, 1), (2, 3), (4, 5), (6, 7)
    near, direct, shared = xs + ys, (2, 4), (3, 5)
    for r in head:
        prepare(r, (0,))
    with jax.named_scope("sib"):
        siblings().wait_recv()
    for r in head:
        prepare(r, (1,))
    def finish(products, settled):
        done = 0
        for i, (slots, n) in enumerate(products):
            last_part(slots, n)
            until = len(settled) * (i + 1) // len(products)
            for pair, m in settled[done:until]:
                settle(pair, m)
            done = until

    own_block(0)
    own_block(1)
    settle(own, 0)
    own_block(2)
    settle(own, 1)
    with jax.named_scope("piece"):
        take_piece(0)
    prepare(0, direct, cuts[0])
    for n in range(3):
        first_part(direct, n, cuts[0])
    own_block(3)
    settle(own, 2)
    with jax.named_scope("take0"):
        take_piece(1)
        onward_y(0).start()
        relay_x(0).start()
    prepare(0, direct, cuts[1])
    for n in range(3):
        first_part(direct, n, cuts[1])
    first_part(direct, 3)
    settle(own, 3)
    own_block(4)
    with jax.named_scope("got0"):
        arrived((0, 3), (0, 5))
    prepare(0, shared)
    first_part(shared, 0)
    settle(own, 4)
    for n in range(1, half):
        first_part(shared, n)
    first_part(near, 4)
    with jax.named_scope("take1"):
        take((1, 2), (1, 4))
        onward_y(1).start()
        relay_x(1).start()
        for r in range(HALF, CHUNKS):
            to_y(r).start()
        panel_copy(5).wait()
        panel_copy(6).wait()
    first_part(own + near, 5)
    first_part(own + near, 6)
    prepare(1, direct)
    last_part(direct, 0)
    last_part(direct, 1)
    with jax.named_scope("take2"):
        take((2, 2), (0, 6))
        arrived((1, 3), (1, 5))
        panel_copy(7).wait()
    first_part(own + near, 7)
    prepare(1, shared)
    last_part(shared, 0)
    last_part(shared, 1)
    steps = [(pair, n) for n in range(5) for pair in (xs, ys)]
    finish(steps[4:], steps[:8])
    with jax.named_scope("take3"):
        take((3, 2), (1, 6))
        arrived((0, 7),)
        both_layers(ready.at[0])
    prepare(0, far)
    for n in range(PANELS):
        first_part(far, n)
    steps = [(pair, n) for n in (5, 6, 7) for pair in (own, xs, ys)]
    finish(steps[:3], [(own, 5)])
    with jax.named_scope("take4"):
        take((2, 4), (2, 6))
    finish(steps[3:], [(own, 6), (own, 7)])
    with jax.named_scope("take5"):
        take((3, 4), (3, 6))
        arrived((1, 7),)
        arrived((2, 3), (3, 3))
        arrived((2, 5), (2, 7))
        pass_ready(1)
    prepare(1, far)
    steps = [(far, n) for n in range(PANELS)]
    finish(steps[:1], [(xs, 4)])
    late_steps = [(ys, 4), (far, 0), (xs, 5), (far, 1), (ys, 5), (far, 2), (xs, 6), (far, 3), (xs, 7)]
    finish(steps[1:5], late_steps)
    with jax.named_scope("last3"):
        arrived((3, 5), (3, 7))
        for step in range(2, count_pb - 1):
            pass_ready(step)
    finish(steps[5:], [(far, 4), (ys, 6), (far, 5), (ys, 7), (far, 6)])
    early = spectra(range(6))
    settle(far, 7)
    late = spectra(far)
    parts[0, 0:1] = -jnp.sum(early[1] + late[1], axis=0, keepdims=True)
    parts[0, 1:2] = jnp.sum(early[0] + late[0], axis=0, keepdims=True)
    with jax.named_scope("ready"):
        pl.semaphore_wait(ready.at[count_pb - 2], layers)
    me = owner(0)
    down = qpoint < count_pb // 2
    for turn in range(count_pb):
        if turn < count_pb - 1:
            high, low = count_pb - 1 - turn, turn
            high = jnp.where(high > qpoint, high, high - 1)
            low = jnp.where(low < qpoint, low, low + 1)
            layer = jnp.where(down, high, low)
        else:
            layer = qpoint
        turned = (layer + count_pb - qpoint) % count_pb * group
        for step in range(group - 1, -1, -1):
            if turn == count_pb - 1 and step == 0:
                continue
            spot = (me + step) % group
            pltpu.make_async_remote_copy(
                src_ref=parts.at[0],
                dst_ref=parts.at[turned + step],
                send_sem=part_send,
                recv_sem=part_recv,
                device_id={"pb": layer, "freq": spot // count_ga, "ga": spot % count_ga},
                device_id_type=MESH,
            ).start()
    with jax.named_scope("drain"):
        for r in range(CHUNKS):
            all_sent(r)
    others = pltpu.make_async_remote_copy(
        src_ref=parts.at[1:],
        dst_ref=parts.at[1:],
        send_sem=part_send,
        recv_sem=part_recv,
        device_id=at_core,
        device_id_type=MESH,
    )
    with jax.named_scope("exch"):
        others.wait_recv()
    total = jnp.sum(parts[...], axis=0)
    first = (qpoint * count_freq + freq) * OUT_DEV
    lanes = lax.broadcasted_iota(jnp.int32, total.shape, 1)
    spots = lax.broadcasted_iota(jnp.int32, (2, OUT_DEV), 1)
    result = jnp.zeros((2, OUT_DEV), jnp.float32)
    for j in range(OUT_DEV):
        picked = jnp.sum(jnp.where(lanes == first + j, total, 0.0), axis=1, keepdims=True)
        result = jnp.where(spots == j, picked, result)
    out_ref[...] = result.reshape(out_ref.shape)
    with jax.named_scope("sent"):
        others.wait_send()


def fused_body(densities, screened, energies, occupied, kmq, offsets, weights):
    count_pb = lax.axis_size("pb")
    count_freq = lax.axis_size("freq")
    count_ga = lax.axis_size("ga")
    pair_rows, basis = densities.shape[2:]
    panel_rows = screened.shape[3]
    group = count_freq * count_ga
    width = basis // CHUNKS
    cols = basis // PANELS
    total_out = OUT_DEV * count_pb * count_freq
    shape = (count_pb, count_freq, count_ga)
    anywhere = pl.BlockSpec(memory_space=pltpu.HBM)
    vector = pl.BlockSpec(memory_space=pltpu.VMEM)
    return pl.pallas_call(
        functools.partial(fused_kernel, shape),
        out_shape=jax.ShapeDtypeStruct((2, NS, OUT_DEV), jnp.float32),
        in_specs=[anywhere] * 7,
        out_specs=vector,
        scratch_shapes=[
            pltpu.VMEM((CHUNKS, SLOTS, 2, pair_rows, width), jnp.bfloat16),
            pltpu.VMEM((HALF, SLOTS, pair_rows, width), jnp.bfloat16),
            pltpu.VMEM((PANELS, 2, panel_rows, cols), jnp.bfloat16),
            pltpu.VMEM((PANELS, SLOTS, 2 * pair_rows, cols), jnp.float32),
            pltpu.VMEM((2, SLOTS, pair_rows, 128), jnp.float32),
            pltpu.VMEM((2, NB, total_out), jnp.float32),
            pltpu.VMEM((count_pb * group, 2, total_out), jnp.float32),
            pltpu.VMEM(energies.shape, energies.dtype),
            pltpu.SMEM(occupied.shape, occupied.dtype),
            pltpu.SMEM(kmq.shape, kmq.dtype),
            pltpu.SMEM(offsets.shape, offsets.dtype),
            pltpu.SMEM(weights.shape, weights.dtype),
            pltpu.SemaphoreType.DMA,
            pltpu.SemaphoreType.DMA((PANELS,)),
            pltpu.SemaphoreType.DMA((5,)),
            pltpu.SemaphoreType.DMA((CHUNKS,)),
            pltpu.SemaphoreType.DMA((14,)),
            pltpu.SemaphoreType.DMA,
            pltpu.SemaphoreType.DMA,
            pltpu.SemaphoreType.DMA,
            pltpu.SemaphoreType.REGULAR((count_pb - 1,)),
        ],
        compiler_params=pltpu.CompilerParams(
            collective_id=0, has_side_effects=True, vmem_limit_bytes=50 * 2**20
        ),
    )(
        *(
            pltpu.with_memory_space_constraint(operand, pltpu.HBM)
            for operand in (densities, screened, energies, occupied, kmq, offsets, weights)
        )
    )


def body(densities, screened, *rest):
    basis, panel_rows = densities.shape[3], screened.shape[3]
    chips = lax.axis_size("freq") == 4 and lax.axis_size("ga") == 2 and lax.axis_size("pb") > 1
    fits = densities.shape[2] % 16 == 0 and basis % (PANELS * 128) == 0 and panel_rows * 2 == basis
    if chips and fits:
        return fused_body(densities, screened, *rest)
    return plain_body(densities, screened, *rest)


def solution(mesh):
    placed = (
        P("pb", None, ("freq", "ga"), None),
        P("pb", "freq", None, "ga", None),
        P(),
        P(),
        P(),
        P(),
        P(),
    )
    return jax.shard_map(
        body, mesh=mesh, in_specs=placed, out_specs=P(None, None, ("pb", "freq")), check_vma=False
    )
```
